128 devices in a mesh: sph: 16 (over x_lo, z, core), rad: 8 (over y, x_hi).
Axes of the slice: x: 4 (x_hi: 2, x_lo: 2; x = x_hi * 2 + x_lo), y: 4, z: 4, core: 2. Of those that a mesh axis runs over, the one named last changes fastest.
Arguments:
- coeffs: bfloat16 [65536, 480], P('sph'), may hold values from -6 to 6
- interp: bfloat16 [65536, 2048], P('sph', 'rad'), may hold values from -0.055664062 to 0.055664062
- phases: float32 [64, 2048], P(None, 'rad'), may hold values from 0.3 to 3
- tables: bfloat16 [16, 480, 480], P('rad'), may hold values from -0.25 to 0.25
- bins: int32 [65536], P('sph'), may hold values from 0 to 63
Outputs:
- fields: bfloat16 [65536, 480], P('sph', 'rad')
The draws below stay inside these ranges and needn't reach their ends.
All inputs are finite; a program needn't handle non-finite values.
Results may differ from the reference program's by a relative error of at most 0.024.
Values may be sent and summed in bfloat16 or wider, within the bound.
No kernel may reach another device: no remote copies, remote signals or barrier semaphores. Data moves between devices by JAX's collectives and lax.ppermute only.
A program may use at most 64 MiB of HBM per device.

```python
import math
import jax
import jax.numpy as jnp
from jax import lax

C = 240
C2 = 480
R = 2048
TBL = 128
NB = 16
NH = 64
S_DEV = 4096
S = 65536
N_SPH = 16


def with_ends(drawn, key, low, top_value):
    longest = drawn.shape.index(max(drawn.shape))
    spots = []
    for shift in (0, 1):
        where = [jax.random.randint(jax.random.fold_in(key, axis), (), 0, length) for axis, length in enumerate(drawn.shape)]
        where[longest] = (where[longest] + shift) % drawn.shape[longest]
        spots.append(tuple(where))
    return drawn.at[spots[0]].set(low).at[spots[1]].set(top_value)


def steps_of(own_key, dims, pieces, low, high):
    def one(axis_at, blocks):
        draws = jax.random.uniform(jax.random.fold_in(jax.random.fold_in(own_key, 6), axis_at), (blocks,), jnp.float32, low / len(pieces), high / len(pieces))
        return jnp.repeat(jnp.exp(draws), dims[axis_at] // blocks).reshape((-1,) + (1,) * (len(dims) - axis_at - 1))

    factor_of = one(*pieces[0])
    for cut in pieces[1:]:
        factor_of = factor_of * one(*cut)
    return factor_of


def noise(key, shape, deviation, reach, pieces=(), held_as=jnp.bfloat16):
    entries = deviation * jax.random.normal(key, shape, jnp.float32)
    if pieces:
        entries = entries * steps_of(key, shape, pieces, -0.22, 0.18)
    return jnp.clip(entries, -reach, reach).astype(held_as)


def setup_inputs(seed: int = 0) -> dict:
    arg_keys = jax.random.split(jax.random.key(seed), 6)
    return {
        "coeffs": noise(arg_keys[0], (S, C2), 1.0, 6.0, ((0, 16),)),
        "interp": noise(arg_keys[1], (S, R), ((S_DEV * N_SPH * R) ** -0.25), 0.055664062, ((0, 16), (1, 8))),
        "phases": jnp.clip(jnp.exp(math.log(3.0) - 2.3025851 * jax.random.uniform(arg_keys[2], (NH, R), jnp.float32) ** steps_of(arg_keys[2], (NH, R), ((1, 8),), -0.2, 0.2)), 0.3, 3.0),
        "tables": noise(arg_keys[3], (NB, C2, C2), (2 * C) ** -0.5, 0.25, ((0, 8),)),
        "bins": with_ends(jax.random.randint(arg_keys[4], (S,), 0, NH), jax.random.fold_in(arg_keys[4], 1), 0, NH - 1).astype(jnp.int32),
    }


def reference(coeffs, interp, phases, tables, bins):
    lifted = phases[bins]
    proj = (interp.astype(jnp.float32) * lifted).astype(jnp.bfloat16)
    nodes_sum = jnp.dot(proj.T, coeffs, preferred_element_type=jnp.float32)
    nodes = nodes_sum.astype(jnp.bfloat16)
    blocks = nodes.reshape(tables.shape[0], TBL, tables.shape[1]).astype(jnp.float32)
    angular = jnp.einsum("btc,bcd->btd", blocks, tables.astype(jnp.float32), precision=lax.Precision.HIGHEST)
    angular = angular.reshape(nodes.shape[0], nodes.shape[1]).astype(jnp.bfloat16)
    return jnp.dot(proj, angular, preferred_element_type=jnp.float32).astype(jnp.bfloat16)
```

```python
import jax
import jax.numpy as jnp
from jax import lax
from jax.experimental import pallas as pl
from jax.experimental.pallas import tpu as pltpu
from jax.sharding import Mesh
from jax.sharding import PartitionSpec as P


SWAP = [(0, 1), (1, 0)]
F32, BF16 = jnp.float32, jnp.bfloat16
HBM = pl.BlockSpec(memory_space=pltpu.HBM)
VM = pl.BlockSpec(memory_space=pltpu.VMEM)


def dot(a, b, ca, cb):
    return lax.dot_general(a, b, (((ca,), (cb,)), ((), ())), preferred_element_type=F32)


def lift_kernel(bins, phases, interp, coeffs, p0, p1, p2, p3, keep, give, iv, cv, isem, csem):
    ny = lax.axis_size("y")
    y = lax.axis_index("y")
    core = lax.axis_index("core")
    chunk = iv.shape[1]
    half = keep.shape[0]
    outs = (p0, p1, p2, p3)
    order = (1, 3, 2, 0)
    reads = []
    for n, k in enumerate(order):
        at = pl.multiple_of(((y + k) % ny) * chunk, chunk)
        ri = pltpu.make_async_copy(interp.at[pl.ds(at, chunk)], iv.at[n], isem.at[n])
        rc = pltpu.make_async_copy(coeffs.at[:, pl.ds(at, chunk)], cv.at[n], csem.at[n])
        ri.start()
        rc.start()
        reads.append((ri, rc, at))
    mine = pl.multiple_of(core * half, half)
    other = pl.multiple_of((1 - core) * half, half)
    ph = jnp.concatenate([phases[:, pl.ds(mine, half)], phases[:, pl.ds(other, half)]], axis=1)
    hi = ph.astype(BF16)
    lo = (ph - hi.astype(F32)).astype(BF16)
    both = jnp.concatenate([hi, lo], axis=0)
    nh = ph.shape[0]
    acc = jnp.zeros((cv.shape[1], 2 * half), F32)
    for n, k in enumerate(order):
        ri, rc, at = reads[n]
        b = bins[:, pl.ds(at, chunk)]
        row = lax.broadcasted_iota(jnp.int32, (nh, chunk), 0)
        one = jnp.where(row == b, 1.0, 0.0).astype(F32)
        one = jnp.concatenate([one, one], axis=0).astype(BF16)
        lifted = dot(one, both, 0, 0)
        ri.wait()
        x = jnp.concatenate([iv[n, :, pl.ds(mine, half)], iv[n, :, pl.ds(other, half)]], axis=1)
        proj = (x.astype(F32) * lifted).astype(BF16)
        outs[k][...] = proj
        rc.wait()
        acc = acc + dot(cv[n], proj, 1, 0)
    nodes = acc.T.astype(BF16)
    keep[...] = nodes[:half]
    give[...] = nodes[half:]


def lift(bins, phases, interp, coeffs_t):
    spheres, rows = interp.shape
    cols = coeffs_t.shape[0]
    chunk = spheres // 4
    piece = pltpu.VMEM((chunk, rows), BF16)
    part = pltpu.VMEM((rows // 2, cols), BF16)
    return pl.pallas_call(
        lift_kernel,
        in_specs=[VM, VM, HBM, HBM],
        out_specs=[VM] * 6,
        out_shape=[piece] * 4 + [part] * 2,
        scratch_shapes=[
            pltpu.VMEM((4, chunk, rows), BF16),
            pltpu.VMEM((4, cols, chunk), BF16),
            pltpu.SemaphoreType.DMA((4,)),
            pltpu.SemaphoreType.DMA((4,)),
        ],
        compiler_params=pltpu.CompilerParams(vmem_limit_bytes=20 << 20),
        name="lift",
    )(vmem(bins), vmem(phases), hbm(interp), hbm(coeffs_t))


def fields_kernel(mine, theirs, p0, p1, p2, p3, out):
    ny = lax.axis_size("y")
    y = lax.axis_index("y")
    acc = None
    for k, p in enumerate((p0, p1, p2, p3)):
        src = (y + ny - k) % ny
        a = jnp.concatenate([mine[src], theirs[src]], axis=0)
        f = dot(a, p[...], 0, 1)
        acc = f if acc is None else acc + f
    out[...] = acc.astype(BF16).reshape(out.shape)


def fields(mine, theirs, pieces, nrad):
    width = mine.shape[2]
    chunk = pieces[0].shape[0]
    return pl.pallas_call(
        fields_kernel,
        in_specs=[VM] * 6,
        out_specs=VM,
        out_shape=pltpu.VMEM((nrad, width // nrad, chunk), BF16),
        compiler_params=pltpu.CompilerParams(vmem_limit_bytes=16 << 20),
        name="fields",
    )(*[vmem(a) for a in (mine, theirs, *pieces)])


def finish_kernel(back, out):
    used = out.shape[0]
    chunk = back.shape[2]
    for j in range(back.shape[0] // 2):
        s = back[2 * j].astype(F32) + back[2 * j + 1].astype(F32)
        out[:, j * chunk : (j + 1) * chunk] = s[:used].astype(BF16)


def finish(back, used):
    total = back.shape[0] // 2 * back.shape[2]
    return pl.pallas_call(
        finish_kernel,
        in_specs=[VM],
        out_specs=VM,
        out_shape=jax.ShapeDtypeStruct((used, total), BF16),
        compiler_params=pltpu.CompilerParams(vmem_limit_bytes=8 << 20),
        name="finish",
    )(vmem(back))


def vmem(a):
    return pltpu.with_memory_space_constraint(a, pltpu.VMEM)


def hbm(a):
    return pltpu.with_memory_space_constraint(a, pltpu.HBM)


def exchange(pieces, axis):
    return lax.all_to_all(pieces, axis, split_axis=0, concat_axis=0, tiled=True)


def steps(coeffs, interp, phases, tables, bins):
    spheres, rows = interp.shape
    cols = coeffs.shape[1]
    ny = lax.axis_size("y")
    chips = lax.axis_size("chip")
    nrad = ny * lax.axis_size("xhi")
    core = lax.axis_index("core")
    half = rows // 2
    used = cols // nrad
    slot = -(-used // 16) * 16
    table = lax.dynamic_index_in_dim(tables, core, 0, keepdims=False)
    table = jnp.pad(table.reshape(cols, nrad, used), ((0, 0), (0, 0), (0, slot - used)))
    table = table.reshape(cols, nrad * slot)
    p0, p1, p2, p3, keep, give = lift(bins.reshape(1, spheres), phases, interp, coeffs.T)
    got = lax.ppermute(give, "core", SWAP)
    pieces = [p0] + [
        lax.ppermute(p, "y", [(i, (i + k) % ny) for i in range(ny)])
        for k, p in ((1, p1), (2, p2), (3, p3))
    ]
    chip_sum = (keep.astype(F32) + got.astype(F32)).astype(BF16)
    arrived = exchange(chip_sum.reshape(chips, half // chips, cols), "chip")
    share = arrived.astype(F32).sum(axis=0).astype(BF16)
    part = jnp.dot(share, table, preferred_element_type=F32).astype(BF16)
    mine = jnp.broadcast_to(part, (ny * chips, *part.shape))
    mine = exchange(mine, ("y", "chip"))
    mine = mine.reshape(ny, half, nrad * slot)
    theirs = lax.ppermute(mine, "core", SWAP)
    f = fields(mine, theirs, pieces, nrad)
    back = exchange(f, ("y", "xhi"))
    return finish(back, used).T


def solution(mesh):
    fine = Mesh(mesh.devices.reshape(8, 2, 4, 2), ("chip", "core", "y", "xhi"))
    sph, rad = ("chip", "core"), ("y", "xhi")
    return jax.shard_map(
        steps,
        mesh=fine,
        in_specs=(P(sph, None), P(sph, rad), P(None, rad), P(rad, None, None), P(sph)),
        out_specs=P(sph, rad),
        check_vma=False,
    )
```

```python
import functools

import jax
import jax.numpy as jnp
from jax import lax
from jax.experimental import pallas as pl
from jax.experimental.pallas import tpu as pltpu
from jax.sharding import Mesh
from jax.sharding import PartitionSpec as P


SWAP = [(0, 1), (1, 0)]
F32, BF16 = jnp.float32, jnp.bfloat16
HBM = pl.BlockSpec(memory_space=pltpu.HBM)
VM = pl.BlockSpec(memory_space=pltpu.VMEM)


def dot(a, b, ca, cb):
    return lax.dot_general(a, b, (((ca,), (cb,)), ((), ())), preferred_element_type=F32)


def lift_kernel(bins_h, phases_h, interp, coeffs, p0, p1, p2, p3, keep, give, bins, phases, iv, cv, pv, isem, csem, osem, ssem):
    ny = lax.axis_size("y")
    y = lax.axis_index("y")
    core = lax.axis_index("core")
    chunk = iv.shape[1]
    half = keep.shape[0]
    outs = (p0, p1, p2, p3)
    order = (1, 3, 2, 0)
    writes = []
    small = [
        pltpu.make_async_copy(bins_h, bins, ssem.at[0]),
        pltpu.make_async_copy(phases_h, phases, ssem.at[1]),
    ]
    for c in small:
        c.start()
    reads = []
    for n, k in enumerate(order):
        at = pl.multiple_of(((y + k) % ny) * chunk, chunk)
        ri = pltpu.make_async_copy(interp.at[pl.ds(at, chunk)], iv.at[n], isem.at[n])
        rc = pltpu.make_async_copy(coeffs.at[:, pl.ds(at, chunk)], cv.at[n], csem.at[n])
        ri.start()
        rc.start()
        reads.append((ri, rc, at))
    for c in small:
        c.wait()
    mine = pl.multiple_of(core * half, half)
    other = pl.multiple_of((1 - core) * half, half)
    ph = jnp.concatenate([phases[:, pl.ds(mine, half)], phases[:, pl.ds(other, half)]], axis=1)
    hi = ph.astype(BF16)
    lo = (ph - hi.astype(F32)).astype(BF16)
    both = jnp.concatenate([hi, lo], axis=0)
    nh = ph.shape[0]
    acc = jnp.zeros((cv.shape[1], 2 * half), F32)
    for n, k in enumerate(order):
        ri, rc, at = reads[n]
        b = bins[:, pl.ds(at, chunk)]
        row = lax.broadcasted_iota(jnp.int32, (nh, chunk), 0)
        one = jnp.where(row == b, 1.0, 0.0).astype(F32)
        one = jnp.concatenate([one, one], axis=0).astype(BF16)
        lifted = dot(one, both, 0, 0)
        ri.wait()
        x = jnp.concatenate([iv[n, :, pl.ds(mine, half)], iv[n, :, pl.ds(other, half)]], axis=1)
        proj = (x.astype(F32) * lifted).astype(BF16)
        if k == 0:
            p0[...] = proj
        else:
            pv[n] = proj
            w = pltpu.make_async_copy(pv.at[n], outs[k], osem.at[n])
            w.start()
            writes.append(w)
        rc.wait()
        acc = acc + dot(cv[n], proj, 1, 0)
    nodes = acc.T.astype(BF16)
    keep[...] = nodes[:half]
    give[...] = nodes[half:]
    for w in writes:
        w.wait()


def lift(bins, phases, interp, coeffs_t):
    spheres, rows = interp.shape
    cols = coeffs_t.shape[0]
    chunk = spheres // 4
    away = pltpu.HBM((chunk, rows), BF16)
    home = pltpu.VMEM((chunk, rows), BF16)
    part = pltpu.VMEM((rows // 2, cols), BF16)
    return pl.pallas_call(
        lift_kernel,
        in_specs=[HBM] * 4,
        out_specs=[VM] + [HBM] * 3 + [VM] * 2,
        out_shape=[home] + [away] * 3 + [part] * 2,
        scratch_shapes=[
            pltpu.VMEM(bins.shape, bins.dtype),
            pltpu.VMEM(phases.shape, phases.dtype),
            pltpu.VMEM((4, chunk, rows), BF16),
            pltpu.VMEM((4, cols, chunk), BF16),
            pltpu.VMEM((3, chunk, rows), BF16),
            pltpu.SemaphoreType.DMA((4,)),
            pltpu.SemaphoreType.DMA((4,)),
            pltpu.SemaphoreType.DMA((3,)),
            pltpu.SemaphoreType.DMA((2,)),
        ],
        compiler_params=pltpu.CompilerParams(vmem_limit_bytes=20 << 20),
        name="lift",
    )(hbm(bins), hbm(phases), hbm(interp), hbm(coeffs_t))


def angular_kernel(arrived, tables, out, *, nrad):
    share = arrived[0].astype(F32)
    for j in range(1, arrived.shape[0]):
        share = share + arrived[j].astype(F32)
    table = tables[lax.axis_index("core")]
    part = dot(share.astype(BF16), table, 1, 0).astype(BF16)
    cols = table.shape[1]
    used, slot = cols // nrad, out.shape[2] // nrad
    src = lax.broadcasted_iota(jnp.int32, (cols, nrad * slot), 0)
    dst = lax.broadcasted_iota(jnp.int32, (cols, nrad * slot), 1)
    at, within = dst // slot, dst % slot
    pick = jnp.where((within < used) & (src == at * used + within), 1.0, 0.0).astype(BF16)
    spread = dot(part, pick, 1, 0).astype(BF16)
    out[...] = jnp.broadcast_to(spread[None], out.shape)


def angular(arrived, tables, copies, nrad, slot):
    rows = arrived.shape[1]
    return pl.pallas_call(
        functools.partial(angular_kernel, nrad=nrad),
        in_specs=[VM] * 2,
        out_specs=VM,
        out_shape=pltpu.VMEM((copies, rows, nrad * slot), BF16),
        compiler_params=pltpu.CompilerParams(vmem_limit_bytes=8 << 20),
        name="angular",
    )(vmem(arrived), vmem(tables))


def fields_kernel(mine, theirs, p0, p1, p2, p3, out):
    ny = lax.axis_size("y")
    y = lax.axis_index("y")
    acc = None
    for k, p in enumerate((p0, p1, p2, p3)):
        src = (y + ny - k) % ny
        a = jnp.concatenate([mine[src], theirs[src]], axis=0)
        f = dot(a, p[...], 0, 1)
        acc = f if acc is None else acc + f
    out[...] = acc.astype(BF16).reshape(out.shape)


def fields(mine, theirs, pieces, nrad):
    width = mine.shape[2]
    chunk = pieces[0].shape[0]
    return pl.pallas_call(
        fields_kernel,
        in_specs=[VM] * 6,
        out_specs=VM,
        out_shape=pltpu.VMEM((nrad, width // nrad, chunk), BF16),
        compiler_params=pltpu.CompilerParams(vmem_limit_bytes=16 << 20),
        name="fields",
    )(*[vmem(a) for a in (mine, theirs, *pieces)])


def finish_kernel(back, out):
    used = out.shape[0]
    chunk = back.shape[2]
    for j in range(back.shape[0] // 2):
        s = back[2 * j].astype(F32) + back[2 * j + 1].astype(F32)
        out[:, j * chunk : (j + 1) * chunk] = s[:used].astype(BF16)


def finish(back, used):
    total = back.shape[0] // 2 * back.shape[2]
    return pl.pallas_call(
        finish_kernel,
        in_specs=[VM],
        out_specs=VM,
        out_shape=jax.ShapeDtypeStruct((used, total), BF16),
        compiler_params=pltpu.CompilerParams(vmem_limit_bytes=8 << 20),
        name="finish",
    )(vmem(back))


def vmem(a):
    return pltpu.with_memory_space_constraint(a, pltpu.VMEM)


def hbm(a):
    return pltpu.with_memory_space_constraint(a, pltpu.HBM)


def exchange(pieces, axis):
    return lax.all_to_all(pieces, axis, split_axis=0, concat_axis=0, tiled=True)


def steps(coeffs, interp, phases, tables, bins):
    spheres, rows = interp.shape
    cols = coeffs.shape[1]
    ny = lax.axis_size("y")
    chips = lax.axis_size("chip")
    nrad = ny * lax.axis_size("xhi")
    half = rows // 2
    used = cols // nrad
    slot = -(-used // 16) * 16
    p0, p1, p2, p3, keep, give = lift(bins.reshape(1, spheres), phases, interp, coeffs.T)
    got = lax.ppermute(give, "core", SWAP)
    pieces = [p0] + [
        lax.ppermute(p, "y", [(i, (i + k) % ny) for i in range(ny)])
        for k, p in ((1, p1), (2, p2), (3, p3))
    ]
    chip_sum = (keep.astype(F32) + got.astype(F32)).astype(BF16)
    arrived = exchange(chip_sum.reshape(chips, half // chips, cols), "chip")
    mine = angular(arrived, tables, ny * chips, nrad, slot)
    mine = exchange(mine, ("y", "chip"))
    mine = mine.reshape(ny, half, nrad * slot)
    theirs = lax.ppermute(mine, "core", SWAP)
    f = fields(mine, theirs, pieces, nrad)
    back = exchange(f, ("y", "xhi"))
    return finish(back, used).T


def solution(mesh):
    fine = Mesh(mesh.devices.reshape(8, 2, 4, 2), ("chip", "core", "y", "xhi"))
    sph, rad = ("chip", "core"), ("y", "xhi")
    return jax.shard_map(
        steps,
        mesh=fine,
        in_specs=(P(sph, None), P(sph, rad), P(None, rad), P(rad, None, None), P(sph)),
        out_specs=P(sph, rad),
        check_vma=False,
    )
```

```python
import functools

import jax
import jax.numpy as jnp
from jax import lax
from jax.experimental import pallas as pl
from jax.experimental.pallas import tpu as pltpu
from jax.sharding import Mesh
from jax.sharding import PartitionSpec as P


SWAP = [(0, 1), (1, 0)]
F32, BF16 = jnp.float32, jnp.bfloat16
HBM = pl.BlockSpec(memory_space=pltpu.HBM)
VM = pl.BlockSpec(memory_space=pltpu.VMEM)


def dot(a, b, ca, cb):
    return lax.dot_general(a, b, (((ca,), (cb,)), ((), ())), preferred_element_type=F32)


def lift_kernel(bins_h, phases_h, interp, q, p1, p2, p3, bins, phases, iv, isem, osem, ssem):
    ny = lax.axis_size("y")
    y = lax.axis_index("y")
    core = lax.axis_index("core")
    chunk = iv.shape[1]
    half = iv.shape[2] // 2
    outs = (None, p1, p2, p3)
    order = (1, 3, 2, 0)
    small = [
        pltpu.make_async_copy(bins_h, bins, ssem.at[0]),
        pltpu.make_async_copy(phases_h, phases, ssem.at[1]),
    ]
    for c in small:
        c.start()
    reads = []
    for n, k in enumerate(order):
        at = pl.multiple_of(((y + k) % ny) * chunk, chunk)
        r = pltpu.make_async_copy(interp.at[pl.ds(at, chunk)], iv.at[n], isem.at[n])
        r.start()
        reads.append((r, at))
    for c in small:
        c.wait()
    mine = pl.multiple_of(core * half, half)
    other = pl.multiple_of((1 - core) * half, half)
    ph = jnp.concatenate([phases[:, pl.ds(mine, half)], phases[:, pl.ds(other, half)]], axis=1)
    hi = ph.astype(BF16)
    lo = (ph - hi.astype(F32)).astype(BF16)
    both = jnp.concatenate([hi, lo], axis=0)
    nh = ph.shape[0]
    writes = []
    for n, k in enumerate(order):
        r, at = reads[n]
        b = bins[:, pl.ds(at, chunk)]
        row = lax.broadcasted_iota(jnp.int32, (nh, chunk), 0)
        one = jnp.where(row == b, 1.0, 0.0).astype(F32)
        one = jnp.concatenate([one, one], axis=0).astype(BF16)
        lifted = dot(one, both, 0, 0)
        r.wait()
        x = jnp.concatenate([iv[n, :, pl.ds(mine, half)], iv[n, :, pl.ds(other, half)]], axis=1)
        q[pl.ds(at, chunk), :] = (x.astype(F32) * lifted).astype(BF16)
        if k:
            w = pltpu.make_async_copy(q.at[pl.ds(at, chunk)], outs[k], osem.at[n])
            w.start()
            writes.append(w)
    for w in writes:
        w.wait()


def lift(bins, phases, interp):
    spheres, rows = interp.shape
    chunk = spheres // 4
    return pl.pallas_call(
        lift_kernel,
        in_specs=[HBM] * 3,
        out_specs=[VM] + [HBM] * 3,
        out_shape=[pltpu.VMEM((spheres, rows), BF16)] + [pltpu.HBM((chunk, rows), BF16)] * 3,
        scratch_shapes=[
            pltpu.VMEM(bins.shape, bins.dtype),
            pltpu.VMEM(phases.shape, phases.dtype),
            pltpu.VMEM((4, chunk, rows), BF16),
            pltpu.SemaphoreType.DMA((4,)),
            pltpu.SemaphoreType.DMA((3,)),
            pltpu.SemaphoreType.DMA((2,)),
        ],
        compiler_params=pltpu.CompilerParams(vmem_limit_bytes=12 << 20),
        name="lift",
    )(hbm(bins), hbm(phases), hbm(interp))


def nodes_kernel(q, coeffs, keep, give):
    half = keep.shape[0]
    nodes = dot(coeffs[...], q[...], 1, 0).T.astype(BF16)
    keep[...] = nodes[:half]
    give[...] = nodes[half:]


def nodes(q, coeffs_t):
    part = pltpu.VMEM((q.shape[1] // 2, coeffs_t.shape[0]), BF16)
    return pl.pallas_call(
        nodes_kernel,
        in_specs=[VM] * 2,
        out_specs=[VM] * 2,
        out_shape=[part] * 2,
        compiler_params=pltpu.CompilerParams(vmem_limit_bytes=12 << 20),
        name="nodes",
    )(vmem(q), vmem(coeffs_t))


def angular_kernel(arrived, tables, out, *, nrad):
    share = arrived[0].astype(F32)
    for j in range(1, arrived.shape[0]):
        share = share + arrived[j].astype(F32)
    table = tables[lax.axis_index("core")]
    part = dot(share.astype(BF16), table, 1, 0).astype(BF16)
    cols = table.shape[1]
    used, slot = cols // nrad, out.shape[2] // nrad
    src = lax.broadcasted_iota(jnp.int32, (cols, nrad * slot), 0)
    dst = lax.broadcasted_iota(jnp.int32, (cols, nrad * slot), 1)
    at, within = dst // slot, dst % slot
    pick = jnp.where((within < used) & (src == at * used + within), 1.0, 0.0).astype(BF16)
    spread = dot(part, pick, 1, 0).astype(BF16)
    out[...] = jnp.broadcast_to(spread[None], out.shape)


def angular(arrived, tables, copies, nrad, slot):
    rows = arrived.shape[1]
    return pl.pallas_call(
        functools.partial(angular_kernel, nrad=nrad),
        in_specs=[VM] * 2,
        out_specs=VM,
        out_shape=pltpu.VMEM((copies, rows, nrad * slot), BF16),
        compiler_params=pltpu.CompilerParams(vmem_limit_bytes=8 << 20),
        name="angular",
    )(vmem(arrived), vmem(tables))


def fields_kernel(mine, theirs, q, p1, p2, p3, out):
    ny = lax.axis_size("y")
    y = lax.axis_index("y")
    acc = None
    chunk = p1.shape[0]
    own = q[pl.ds(pl.multiple_of(y * chunk, chunk), chunk), :]
    for k, p in enumerate((own, p1, p2, p3)):
        src = (y + ny - k) % ny
        a = jnp.concatenate([mine[src], theirs[src]], axis=0)
        f = dot(a, p[...], 0, 1)
        acc = f if acc is None else acc + f
    out[...] = acc.astype(BF16).reshape(out.shape)


def fields(mine, theirs, pieces, nrad):
    width = mine.shape[2]
    chunk = pieces[1].shape[0]
    return pl.pallas_call(
        fields_kernel,
        in_specs=[VM] * 6,
        out_specs=VM,
        out_shape=pltpu.VMEM((nrad, width // nrad, chunk), BF16),
        compiler_params=pltpu.CompilerParams(vmem_limit_bytes=16 << 20),
        name="fields",
    )(*[vmem(a) for a in (mine, theirs, *pieces)])


def finish_kernel(back, out):
    used = out.shape[0]
    chunk = back.shape[2]
    for j in range(back.shape[0] // 2):
        s = back[2 * j].astype(F32) + back[2 * j + 1].astype(F32)
        out[:, j * chunk : (j + 1) * chunk] = s[:used].astype(BF16)


def finish(back, used):
    total = back.shape[0] // 2 * back.shape[2]
    return pl.pallas_call(
        finish_kernel,
        in_specs=[VM],
        out_specs=VM,
        out_shape=jax.ShapeDtypeStruct((used, total), BF16),
        compiler_params=pltpu.CompilerParams(vmem_limit_bytes=8 << 20),
        name="finish",
    )(vmem(back))


def vmem(a):
    return pltpu.with_memory_space_constraint(a, pltpu.VMEM)


def hbm(a):
    return pltpu.with_memory_space_constraint(a, pltpu.HBM)


def exchange(pieces, axis):
    return lax.all_to_all(pieces, axis, split_axis=0, concat_axis=0, tiled=True)


def steps(coeffs, interp, phases, tables, bins):
    spheres, rows = interp.shape
    cols = coeffs.shape[1]
    ny = lax.axis_size("y")
    chips = lax.axis_size("chip")
    nrad = ny * lax.axis_size("xhi")
    half = rows // 2
    used = cols // nrad
    slot = -(-used // 16) * 16
    q, p1, p2, p3 = lift(bins.reshape(1, spheres), phases, interp)
    keep, give = nodes(q, coeffs.T)
    got = lax.ppermute(give, "core", SWAP)
    pieces = [q] + [
        lax.ppermute(p, "y", [(i, (i + k) % ny) for i in range(ny)])
        for k, p in ((1, p1), (2, p2), (3, p3))
    ]
    chip_sum = (keep.astype(F32) + got.astype(F32)).astype(BF16)
    arrived = exchange(chip_sum.reshape(chips, half // chips, cols), "chip")
    mine = angular(arrived, tables, ny * chips, nrad, slot)
    mine = exchange(mine, ("y", "chip"))
    mine = mine.reshape(ny, half, nrad * slot)
    theirs = lax.ppermute(mine, "core", SWAP)
    f = fields(mine, theirs, pieces, nrad)
    back = exchange(f, ("y", "xhi"))
    return finish(back, used).T


def solution(mesh):
    fine = Mesh(mesh.devices.reshape(8, 2, 4, 2), ("chip", "core", "y", "xhi"))
    sph, rad = ("chip", "core"), ("y", "xhi")
    return jax.shard_map(
        steps,
        mesh=fine,
        in_specs=(P(sph, None), P(sph, rad), P(None, rad), P(rad, None, None), P(sph)),
        out_specs=P(sph, rad),
        check_vma=False,
    )
```

```python
import functools

import jax
import jax.numpy as jnp
from jax import lax
from jax.experimental import pallas as pl
from jax.experimental.pallas import tpu as pltpu
from jax.sharding import Mesh
from jax.sharding import PartitionSpec as P


SWAP = [(0, 1), (1, 0)]
HOPS = ((0, 1), (1, 0), (3, 0), (2, 1), (1, 1), (3, 1), (2, 0), (0, 0))
F32, BF16 = jnp.float32, jnp.bfloat16
HBM = pl.BlockSpec(memory_space=pltpu.HBM)
VM = pl.BlockSpec(memory_space=pltpu.VMEM)


def dot(a, b, ca, cb):
    return lax.dot_general(a, b, (((ca,), (cb,)), ((), ())), preferred_element_type=F32)


def split_phases(phases, core):
    half = phases.shape[1] // 2
    mine = pl.multiple_of(core * half, half)
    other = pl.multiple_of((1 - core) * half, half)
    ph = jnp.concatenate([phases[:, pl.ds(mine, half)], phases[:, pl.ds(other, half)]], axis=1)
    hi = ph.astype(BF16)
    lo = (ph - hi.astype(F32)).astype(BF16)
    return jnp.concatenate([hi, lo], axis=0), mine, other


def lifted_chunk(bins, both, x_ref, mine, other, at, chunk):
    nh, half = both.shape[0] // 2, both.shape[1] // 2
    row = lax.broadcasted_iota(jnp.int32, (nh, chunk), 0)
    one = jnp.where(row == bins[:, pl.ds(at, chunk)], 1.0, 0.0)
    one = jnp.concatenate([one, one], axis=0).astype(BF16)
    lifted = dot(one, both, 0, 0)
    x = jnp.concatenate([x_ref[:, pl.ds(mine, half)], x_ref[:, pl.ds(other, half)]], axis=1)
    return (x.astype(F32) * lifted).astype(BF16)


def lift_kernel(
    bins_h, phases_h, interp, coeffs, p1, p2, p3, raw, cv, bins, phases, iv, isem, csem, ssem
):
    ny = lax.axis_size("y")
    y = lax.axis_index("y")
    core = lax.axis_index("core")
    chunk = raw.shape[0]
    small = [
        pltpu.make_async_copy(bins_h, bins, ssem.at[0]),
        pltpu.make_async_copy(phases_h, phases, ssem.at[1]),
    ]
    for c in small:
        c.start()
    reads = []
    for n, k in enumerate((1, 3, 2, 0)):
        at = pl.multiple_of(((y + k) % ny) * chunk, chunk)
        to = iv.at[n] if k else raw
        r = pltpu.make_async_copy(interp.at[pl.ds(at, chunk)], to, isem.at[n])
        r.start()
        reads.append((r, at))
    load = pltpu.make_async_copy(coeffs, cv, csem)
    load.start()
    for c in small:
        c.wait()
    both, mine, other = split_phases(phases, core)
    for n, p in enumerate((p1, p3, p2)):
        r, at = reads[n]
        r.wait()
        p[...] = lifted_chunk(bins, both, iv.at[n], mine, other, at, chunk)
    reads[3][0].wait()
    load.wait()


def lift(bins, phases, interp, coeffs_t):
    spheres, rows = interp.shape
    chunk = spheres // 4
    piece = pltpu.VMEM((chunk, rows), BF16)
    return pl.pallas_call(
        lift_kernel,
        in_specs=[HBM] * 4,
        out_specs=[VM] * 5,
        out_shape=[piece] * 4 + [pltpu.VMEM(coeffs_t.shape, BF16)],
        scratch_shapes=[
            pltpu.VMEM(bins.shape, bins.dtype),
            pltpu.VMEM(phases.shape, phases.dtype),
            pltpu.VMEM((3, chunk, rows), BF16),
            pltpu.SemaphoreType.DMA((4,)),
            pltpu.SemaphoreType.DMA(()),
            pltpu.SemaphoreType.DMA((2,)),
        ],
        compiler_params=pltpu.CompilerParams(vmem_limit_bytes=12 << 20),
        name="lift",
    )(hbm(bins), hbm(phases), hbm(interp), hbm(coeffs_t))


def nodes_kernel(bins, phases, p1, p2, p3, raw, coeffs, p0, keep, give):
    ny = lax.axis_size("y")
    y = lax.axis_index("y")
    chunk = raw.shape[0]
    half = keep.shape[0]
    both, mine, other = split_phases(phases, lax.axis_index("core"))
    acc = None
    for k, p in ((1, p1), (3, p3), (2, p2), (0, p0)):
        at = pl.multiple_of(((y + k) % ny) * chunk, chunk)
        if k == 0:
            p[...] = lifted_chunk(bins, both, raw, mine, other, at, chunk)
        part = dot(coeffs[:, pl.ds(at, chunk)], p[...], 1, 0)
        acc = part if acc is None else acc + part
    nodes = acc.T.astype(BF16)
    keep[...] = nodes[:half]
    give[...] = nodes[half:]


def nodes(bins, phases, p1, p2, p3, raw, coeffs_t):
    part = pltpu.VMEM((raw.shape[1] // 2, coeffs_t.shape[0]), BF16)
    return pl.pallas_call(
        nodes_kernel,
        in_specs=[VM] * 7,
        out_specs=[VM] * 3,
        out_shape=[pltpu.VMEM(raw.shape, BF16), part, part],
        compiler_params=pltpu.CompilerParams(vmem_limit_bytes=8 << 20),
        name="nodes",
    )(*[vmem(a) for a in (bins, phases, p1, p2, p3, raw, coeffs_t)])


def angular_kernel(arrived, tables, out, *, nrad):
    share = arrived[0].astype(F32)
    for j in range(1, arrived.shape[0]):
        share = share + arrived[j].astype(F32)
    table = tables[lax.axis_index("core")]
    part = dot(share.astype(BF16), table, 1, 0).astype(BF16)
    cols = table.shape[1]
    used, slot = cols // nrad, out.shape[2] // nrad
    src = lax.broadcasted_iota(jnp.int32, (cols, nrad * slot), 0)
    dst = lax.broadcasted_iota(jnp.int32, (cols, nrad * slot), 1)
    at, within = dst // slot, dst % slot
    pick = jnp.where((within < used) & (src == at * used + within), 1.0, 0.0).astype(BF16)
    spread = dot(part, pick, 1, 0).astype(BF16)
    out[...] = jnp.broadcast_to(spread[None], out.shape)


def angular(arrived, tables, copies, nrad, slot):
    rows = arrived.shape[1]
    return pl.pallas_call(
        functools.partial(angular_kernel, nrad=nrad),
        in_specs=[VM] * 2,
        out_specs=VM,
        out_shape=pltpu.VMEM((copies, rows, nrad * slot), BF16),
        compiler_params=pltpu.CompilerParams(vmem_limit_bytes=8 << 20),
        name="angular",
    )(vmem(arrived), vmem(tables))


def fields_kernel(mine, theirs, p0, p1, p2, p3, *refs):
    outs, f_ref = refs[:-1], refs[-1]
    ny, nx = lax.axis_size("y"), lax.axis_size("xhi")
    y, x = lax.axis_index("y"), lax.axis_index("xhi")
    acc = None
    for k, p in enumerate((p0, p1, p2, p3)):
        src = (y + ny - k) % ny
        a = jnp.concatenate([mine[src], theirs[src]], axis=0)
        f = dot(a, p[...], 0, 1)
        acc = f if acc is None else acc + f
    f_ref[...] = acc.astype(BF16).reshape(f_ref.shape)
    for (dy, dx), out in zip(HOPS, outs):
        out[...] = f_ref[(y + dy) % ny * nx + (x + dx) % nx]


def fields(mine, theirs, pieces, nrad):
    slot = mine.shape[2] // nrad
    chunk = pieces[0].shape[0]
    return pl.pallas_call(
        fields_kernel,
        in_specs=[VM] * 6,
        out_specs=[VM] * nrad,
        out_shape=[pltpu.VMEM((slot, chunk), BF16)] * nrad,
        scratch_shapes=[pltpu.VMEM((nrad, slot, chunk), BF16)],
        compiler_params=pltpu.CompilerParams(vmem_limit_bytes=8 << 20),
        name="fields",
    )(*[vmem(a) for a in (mine, theirs, *pieces)])


def finish_kernel(*refs):
    back, out = dict(zip(HOPS, refs[:-1])), refs[-1]
    ny = lax.axis_size("y")
    y = lax.axis_index("y")
    used = out.shape[0]
    chunk = refs[0].shape[1]
    for dy in range(4):
        s = back[dy, 0][...].astype(F32) + back[dy, 1][...].astype(F32)
        at = pl.multiple_of((y + ny - dy) % ny * chunk, chunk)
        out[:, pl.ds(at, chunk)] = s[:used].astype(BF16)


def finish(back, used):
    total = 4 * back[0].shape[1]
    return pl.pallas_call(
        finish_kernel,
        in_specs=[VM] * len(back),
        out_specs=VM,
        out_shape=jax.ShapeDtypeStruct((used, total), BF16),
        compiler_params=pltpu.CompilerParams(vmem_limit_bytes=8 << 20),
        name="finish",
    )(*[vmem(a) for a in back])


def deliver(piece, dy, dx):
    ny, nx = lax.axis_size("y"), lax.axis_size("xhi")
    if (dy, dx) == (0, 0):
        return piece
    hops = [
        (y * nx + x, (y + dy) % ny * nx + (x + dx) % nx) for y in range(ny) for x in range(nx)
    ]
    return lax.ppermute(piece, ("y", "xhi"), hops)


def vmem(a):
    return pltpu.with_memory_space_constraint(a, pltpu.VMEM)


def hbm(a):
    return pltpu.with_memory_space_constraint(a, pltpu.HBM)


def exchange(pieces, axis):
    return lax.all_to_all(pieces, axis, split_axis=0, concat_axis=0, tiled=True)


def steps(coeffs, interp, phases, tables, bins):
    spheres, rows = interp.shape
    cols = coeffs.shape[1]
    ny = lax.axis_size("y")
    chips = lax.axis_size("chip")
    nrad = ny * lax.axis_size("xhi")
    half = rows // 2
    used = cols // nrad
    slot = -(-used // 16) * 16
    bins = bins.reshape(1, spheres)
    p1, p2, p3, raw, coeffs_t = lift(bins, phases, interp, coeffs.T)
    p0, keep, give = nodes(bins, phases, p1, p2, p3, raw, coeffs_t)
    got = lax.ppermute(give, "core", SWAP)
    pieces = [p0] + [
        lax.ppermute(p, "y", [(i, (i + k) % ny) for i in range(ny)])
        for k, p in ((1, p1), (2, p2), (3, p3))
    ]
    chip_sum = (keep.astype(F32) + got.astype(F32)).astype(BF16)
    arrived = exchange(chip_sum.reshape(chips, half // chips, cols), "chip")
    mine = angular(arrived, tables, ny * chips, nrad, slot)
    mine = exchange(mine, ("y", "chip"))
    mine = mine.reshape(ny, half, nrad * slot)
    theirs = lax.ppermute(mine, "core", SWAP)
    f = fields(mine, theirs, pieces, nrad)
    back = [deliver(piece, dy, dx) for (dy, dx), piece in zip(HOPS, f)]
    return finish(back, used).T


def solution(mesh):
    fine = Mesh(mesh.devices.reshape(8, 2, 4, 2), ("chip", "core", "y", "xhi"))
    sph, rad = ("chip", "core"), ("y", "xhi")
    return jax.shard_map(
        steps,
        mesh=fine,
        in_specs=(P(sph, None), P(sph, rad), P(None, rad), P(rad, None, None), P(sph)),
        out_specs=P(sph, rad),
        check_vma=False,
    )
```
